256 devices in a mesh: kpt: 2 (over y), row: 64 (over z, x), freq: 2 (over core).
Axes of the slice: x: 4, y: 2, z: 16, core: 2. Of those that a mesh axis runs over, the one named last changes fastest.
The devices are a block of a 4x16x16 slice.
Arguments:
- screened: bfloat16 [8, 2, 8192, 8192], P(('kpt', 'freq'), None, 'row'), parts along dimension 0, may hold values from -0.0625 to 0.0625
- elements: bfloat16 [2, 1024, 8192], P(None, 'kpt', 'row'), parts along dimension 1, may hold values from -0.59765625 to 0.59765625
- node_freq: float32 [4], P('freq'), may hold values from 0.1 to 2
- node_weight: float32 [4], P('freq'), may hold values from 0.1 to 1
- band_energy: float32 [1024], P('kpt'), parts along dimension 0, may hold values from -1 to 1
- energy_grid: float32 [64], replicated, may hold values from -1 to 1
- pair_state: int32 [1024], P('kpt'), parts along dimension 0, may hold values from 0 to 31
- pair_band: int32 [1024], P('kpt'), parts along dimension 0, may hold values from 0 to 511
Outputs:
- sigma: float32 [2, 64, 64], P(None, 'kpt'), parts along dimension 1
The draws below stay inside these ranges and needn't reach their ends.
There are 2 independent parts, one for each index of `kpt`. The reference program is written for one: setup_inputs(seed, part) draws one part's arguments, and reference() takes and returns one part's arrays. A program takes and returns all parts, laid end to end along the dimension named above; an argument that names none is the same for every part. Nothing has to cross between parts.
All inputs are finite; a program needn't handle non-finite values.
Results may differ from the reference program's by a relative error of at most 0.0003.
Values may be sent and summed in bfloat16 or wider, within the bound.
No kernel may reach another device: no remote copies, remote signals or barrier semaphores. Data moves between devices by JAX's collectives and lax.ppermute only.
A program may use at most 128 MiB of HBM per device.

```python
import math
import jax
import jax.numpy as jnp

NG = 8192
NPAIR = 512
NBAND = 512
NSTATE = 32
NE = 64
NODES = 4


def place_ends(result, key, low, largest):
    spot = [jax.random.randint(jax.random.fold_in(key, axis), (), 0, length) for axis, length in enumerate(result.shape)]
    main_axis = result.shape.index(max(result.shape))
    neighbour = spot[:main_axis] + [(spot[main_axis] + 1) % result.shape[main_axis]] + spot[main_axis + 1:]
    return result.at[tuple(spot)].set(low).at[tuple(neighbour)].set(largest)


def steps_of(own_key, shape, split, low, high):
    def one(dim, shards_of):
        steps = jax.random.uniform(jax.random.fold_in(jax.random.fold_in(own_key, 6), dim), (shards_of,), jnp.float32, low / len(split), high / len(split))
        return jnp.repeat(jnp.exp(steps), shape[dim] // shards_of).reshape((-1,) + (1,) * (len(shape) - dim - 1))

    loudness = one(*split[0])
    for cut in split[1:]:
        loudness = loudness * one(*cut)
    return loudness


def centred(key, extent, scale, most, shards=(), kind=jnp.bfloat16):
    result = scale * jax.random.normal(key, extent, jnp.float32)
    if shards:
        result = result * steps_of(key, extent, shards, -0.22, 0.18)
    return jnp.clip(result, -most, most).astype(kind)


def setup_inputs(seed: int = 0, part: int = 0) -> dict:
    key_of = jax.random.split(jax.random.key(seed), 9)
    part_splits = jax.random.split(jax.random.fold_in(key_of[8], part), 9)
    return {
        "screened": centred(part_splits[0], (NODES, 2, NG, NG), NG ** -0.5, 0.0625, ((0, 2), (2, 64))),
        "elements": centred(part_splits[1], (2, NPAIR, NG), 0.1, 0.59765625, ((2, 64),)),
        "node_freq": jnp.clip(jnp.exp(math.log(2.0) - 2.9957323 * jax.random.uniform(key_of[2], (NODES,), jnp.float32) ** steps_of(key_of[2], (NODES,), ((0, 2),), -0.2, 0.2)), 0.1, 2.0),
        "node_weight": jnp.clip(jnp.exp(math.log(1.0) - 2.3025851 * jax.random.uniform(key_of[3], (NODES,), jnp.float32) ** steps_of(key_of[3], (NODES,), ((0, 2),), -0.2, 0.2)), 0.1, 1.0),
        "band_energy": jnp.clip(jax.random.uniform(part_splits[4], (NBAND,), jnp.float32, -1.0, 1.0), -1.0, 1.0),
        "energy_grid": jnp.clip(jax.random.uniform(key_of[5], (NE,), jnp.float32, -1.0, 1.0), -1.0, 1.0),
        "pair_state": place_ends(jax.random.randint(part_splits[6], (NPAIR,), 0, NSTATE), jax.random.fold_in(part_splits[6], 1), 0, NSTATE - 1).astype(jnp.int32),
        "pair_band": place_ends(jax.random.randint(part_splits[7], (NPAIR,), 0, NBAND), jax.random.fold_in(part_splits[7], 1), 0, NBAND - 1).astype(jnp.int32),
    }


def reference(screened, elements, node_freq, node_weight, band_energy, energy_grid, pair_state, pair_band):
    real_el = elements[0]
    imag_el = elements[1]
    real_t = real_el.T.astype(jnp.float32)
    imag_t = imag_el.T.astype(jnp.float32)
    forms_re = []
    forms_im = []
    for node in range(NODES):
        w_real = screened[node, 0]
        w_imag = screened[node, 1]
        y_real = jnp.dot(w_real, real_el.T, preferred_element_type=jnp.float32) - jnp.dot(w_imag, imag_el.T, preferred_element_type=jnp.float32)
        y_imag = jnp.dot(w_real, imag_el.T, preferred_element_type=jnp.float32) + jnp.dot(w_imag, real_el.T, preferred_element_type=jnp.float32)
        forms_re.append(jnp.sum(real_t * y_real + imag_t * y_imag, axis=0))
        forms_im.append(jnp.sum(real_t * y_imag - imag_t * y_real, axis=0))
    form_re = jnp.stack(forms_re)
    form_im = jnp.stack(forms_im)
    pair_eps = band_energy[pair_band]
    delta = energy_grid[None, :] - pair_eps[:, None]
    factor = node_weight[:, None, None] * delta[None] / (delta[None] ** 2 + node_freq[:, None, None] ** 2)
    terms_re = jnp.sum(form_re[:, :, None] * factor, axis=0)
    terms_im = jnp.sum(form_im[:, :, None] * factor, axis=0)
    sig_re = jax.ops.segment_sum(terms_re, pair_state, NSTATE)
    sig_im = jax.ops.segment_sum(terms_im, pair_state, NSTATE)
    return jnp.stack([sig_re, sig_im])
```

```python
import functools

import jax
import jax.numpy as jnp
from jax import lax
from jax.experimental import pallas as pl
from jax.experimental.pallas import tpu as pltpu
from jax.sharding import Mesh
from jax.sharding import PartitionSpec as P

NSTATE = 32
ROW = ("row_0", "row_1")
F32 = jnp.float32


def shift(value, axis, step):
    size = lax.axis_size(axis)
    return lax.ppermute(value, axis, [(i, (i + step) % size) for i in range(size)])


def sum_over(value, axis):
    copies = jnp.broadcast_to(value, (lax.axis_size(axis), *value.shape))
    return lax.all_to_all(copies, axis, split_axis=0, concat_axis=0, tiled=True).sum(axis=0)


def block_products(place, w_own, w_other, *refs, blocks, first, last):
    pieces = refs[: 2 * blocks]
    refs = refs[2 * blocks :]
    if not first:
        y_in, refs = refs[0], refs[1:]
    if last:
        own, refs = refs[0], refs[1:]
    out, refs = refs[0], refs[1:]
    w_buf, m_buf, sems = refs[:3]
    y = refs[3] if last else out
    rows, width = w_own.shape[0], w_buf.shape[2]
    columns, lanes = m_buf.shape[1], pieces[0].shape[1]

    copies = []
    for b in range(blocks):
        start = pl.multiple_of(place[b] * width, width)
        for half, w in enumerate((w_own, w_other)):
            copy = pltpu.make_async_copy(
                w.at[:, pl.ds(start, width)],
                w_buf.at[b, pl.ds(half * rows, rows), :],
                sems.at[b, half],
            )
            copy.start()
            copies.append(copy)
    for b in range(blocks):
        for k in range(4):
            lane = pl.multiple_of(place[blocks + k] * lanes, lanes)
            piece = pieces[2 * b + k // 2]
            m_buf[b, :, pl.ds(lane, lanes)] = piece[pl.ds((k % 2) * columns, columns), :]
    for b in range(blocks):
        copies[2 * b].wait()
        copies[2 * b + 1].wait()
        term = lax.dot_general(
            w_buf[b], m_buf[b], (((1,), (1,)), ((), ())), preferred_element_type=F32
        )
        if b == 0:
            y[...] = term if first else y_in[...] + term
        else:
            y[...] += term
    if last:
        pairs, depth = columns // 2, own.shape[1]
        own_re = own[0].astype(F32)
        own_im = own[1].astype(F32)
        for node in range(out.shape[0] // 2):
            base = node * 2 * depth
            w_re = y[pl.ds(base, depth), :]
            w_im = y[pl.ds(base + depth, depth), :]
            y_re = w_re[:, :pairs] - w_im[:, pairs:]
            y_im = w_re[:, pairs:] + w_im[:, :pairs]
            form_re = jnp.sum(own_re * y_re + own_im * y_im, axis=0, keepdims=True)
            form_im = jnp.sum(own_re * y_im - own_im * y_re, axis=0, keepdims=True)
            out[pl.ds(2 * node, 1), :] = form_re
            out[pl.ds(2 * node + 1, 1), :] = form_im


def add_blocks(y, numbers, positions, w_own, w_other, pieces, own=None):
    blocks = len(numbers)
    first, last = y is None, own is not None
    place = jnp.stack([*numbers, *positions]).astype(jnp.int32)
    rows, columns = 2 * w_own.shape[0], pieces[0].shape[0] // 2
    width = 4 * pieces[0].shape[1]
    vmem = pl.BlockSpec(memory_space=pltpu.VMEM)
    hbm = pl.BlockSpec(memory_space=pltpu.HBM)
    operands = [place, w_own, w_other, *pieces]
    specs = [pl.BlockSpec(memory_space=pltpu.SMEM), hbm, hbm, *[vmem] * len(pieces)]
    aliases = {}
    if not first:
        if not last:
            aliases = {len(operands): 0}
        operands.append(y)
        specs.append(vmem)
    if last:
        operands.append(own)
        specs.append(vmem)
        depth = own.shape[1]
        shape = (rows // depth, columns // 2)
    else:
        shape = (rows, columns)
    scratch = [
        pltpu.VMEM((blocks, rows, width), w_own.dtype),
        pltpu.VMEM((blocks, columns, width), pieces[0].dtype),
        pltpu.SemaphoreType.DMA((blocks, 2)),
    ]
    if last:
        scratch.append(pltpu.VMEM((rows, columns), F32))
    flops = 2 * blocks * rows * columns * width
    return pl.pallas_call(
        functools.partial(block_products, blocks=blocks, first=first, last=last),
        out_shape=jax.ShapeDtypeStruct(shape, F32),
        in_specs=specs,
        out_specs=vmem,
        scratch_shapes=scratch,
        input_output_aliases=aliases,
        compiler_params=pltpu.CompilerParams(vmem_limit_bytes=24 * 2**20),
        cost_estimate=pl.CostEstimate(
            flops=flops, bytes_accessed=2 * blocks * rows * width, transcendentals=0
        ),
        name="block_products",
    )(*operands)


def node_factor(node_freq, node_weight, band_energy, energy_grid, pair_band):
    band_onehot = (
        pair_band[:, None] == jnp.arange(band_energy.shape[0], dtype=jnp.int32)[None, :]
    ).astype(F32)
    pair_eps = jnp.dot(band_onehot, band_energy, precision=lax.Precision.HIGHEST)
    delta = energy_grid[None, :] - pair_eps[:, None]
    return (
        node_weight[:, None, None]
        * delta[None]
        / (delta[None] ** 2 + node_freq[:, None, None] ** 2)
    )


def per_device(
    screened, elements, node_freq, node_weight, band_energy, energy_grid, pair_state, pair_band
):
    nodes, _, depth, waves = screened.shape
    npair = elements.shape[1]
    half = npair // lax.axis_size("freq")
    core = lax.axis_index("freq")
    z, x = lax.axis_index("row_0"), lax.axis_index("row_1")
    nz, nx = lax.axis_size("row_0"), lax.axis_size("row_1")

    w_own = screened.reshape(nodes * 2 * depth, waves)
    w_other = shift(w_own, "freq", 1)
    quadrature = jnp.stack([node_freq, node_weight])
    quadrature = jnp.concatenate([quadrature, shift(quadrature, "freq", 1)], axis=1)

    mine = lax.dynamic_slice_in_dim(elements, core * half, half, 1)
    piece = mine.reshape(2 * half, depth)
    before = shift(piece, "row_1", 1)
    after = shift(piece, "row_1", -1)
    across = shift(piece, "row_1", 2)
    positions = [x, (x - 1) % nx, (x + 1) % nx, (x + 2) % nx]

    up = {0: [jnp.concatenate([piece, before]), jnp.concatenate([after, across])]}
    down = {0: up[0]}
    far = nz // 2
    for r in range(1, far):
        up[r] = [shift(v, "row_0", 1) for v in up[r - 1]]
        down[r] = [shift(v, "row_0", -1) for v in down[r - 1]]
    opposite = [shift(up[far - 1][0], "row_0", 1), shift(down[far - 1][1], "row_0", -1)]

    y = None
    for group in ((0, 1), (2, 3), (4, 5), (6, 7)):
        numbers, pieces = [], []
        for r in group:
            numbers.append((z - r) % nz)
            pieces += up[r]
            if r:
                numbers.append((z + r) % nz)
                pieces += down[r]
        y = add_blocks(y, numbers, positions, w_own, w_other, pieces)
    own = mine.transpose(0, 2, 1)
    form = add_blocks(y, [(z + far) % nz], positions, w_own, w_other, opposite, own)

    form = sum_over(sum_over(form, "row_1"), "row_0")
    form = form.reshape(2 * nodes, 2, half)

    my_band = lax.dynamic_slice_in_dim(pair_band, core * half, half, 0)
    my_state = lax.dynamic_slice_in_dim(pair_state, core * half, half, 0)
    factor = node_factor(quadrature[0], quadrature[1], band_energy, energy_grid, my_band)
    terms = jnp.sum(form[:, :, :, None] * factor[:, None], axis=0)
    state_onehot = (
        jnp.arange(NSTATE, dtype=jnp.int32)[:, None] == my_state[None, :]
    ).astype(F32)
    sigma = [jnp.dot(state_onehot, t, precision=lax.Precision.HIGHEST) for t in terms]
    return lax.psum(jnp.stack(sigma), "freq")


def solution(mesh):
    split = Mesh(
        mesh.devices.reshape(mesh.shape["kpt"], 16, 4, mesh.shape["freq"]),
        ("kpt", "row_0", "row_1", "freq"),
    )
    return jax.shard_map(
        per_device,
        mesh=split,
        in_specs=(
            P(("kpt", "freq"), None, ROW, None),
            P(None, "kpt", ROW),
            P("freq"),
            P("freq"),
            P("kpt"),
            P(),
            P("kpt"),
            P("kpt"),
        ),
        out_specs=P(None, "kpt", None),
        check_vma=False,
    )
```

```python
import functools

import jax
import jax.numpy as jnp
from jax import lax
from jax.experimental import pallas as pl
from jax.experimental.pallas import tpu as pltpu
from jax.sharding import Mesh
from jax.sharding import PartitionSpec as P

NSTATE = 32
ROW = ("row_0", "row_1")
F32 = jnp.float32


def shift(value, axis, step):
    size = lax.axis_size(axis)
    return lax.ppermute(value, axis, [(i, (i + step) % size) for i in range(size)])


def sum_over(value, axis):
    copies = jnp.broadcast_to(value, (lax.axis_size(axis), *value.shape))
    return lax.all_to_all(copies, axis, split_axis=0, concat_axis=0, tiled=True).sum(axis=0)


def block_products(place, w_own, w_other, *refs, numbers, first, last):
    blocks = len(numbers)
    pieces = refs[: 2 * blocks]
    refs = refs[2 * blocks :]
    if not first:
        y_in, refs = refs[0], refs[1:]
    if last:
        own, refs = refs[0], refs[1:]
    out, refs = refs[0], refs[1:]
    w_buf, m_buf, sems = refs[:3]
    y = refs[3] if last else out
    rows, width = w_own.shape[0], w_buf.shape[2]
    columns, lanes = m_buf.shape[1], pieces[0].shape[1]

    def copy_of(b, number, half):
        start = pl.multiple_of(place[number] * width, width)
        return pltpu.make_async_copy(
            (w_own, w_other)[half].at[:, pl.ds(start, width)],
            w_buf.at[b, pl.ds(half * rows, rows), :],
            sems.at[b, half],
        )

    for b, number in enumerate(numbers):
        copy_of(b, number, 0).start()
        copy_of(b, number, 1).start()
    for b in range(blocks):
        for k in range(4):
            lane = pl.multiple_of(place[place.shape[0] - 4 + k] * lanes, lanes)
            piece = pieces[2 * b + k // 2]
            m_buf[b, :, pl.ds(lane, lanes)] = piece[pl.ds((k % 2) * columns, columns), :]
    if last:
        flat = own[...].astype(F32).T
        pairs, depth = columns // 2, own.shape[1]
        own_re, own_im = flat[:, :pairs], flat[:, pairs:]

    def product(b):
        return lax.dot_general(
            w_buf[b], m_buf[b], (((1,), (1,)), ((), ())), preferred_element_type=F32
        )

    for b, number in enumerate(numbers):
        copy_of(b, number, 0).wait()
        copy_of(b, number, 1).wait()
        if b == 0:
            y[...] = product(b) if first else y_in[...] + product(b)
        else:
            y[...] += product(b)
    if last:
        for node in range(out.shape[0] // 2):
            base = node * 2 * depth
            w_re = y[pl.ds(base, depth), :]
            w_im = y[pl.ds(base + depth, depth), :]
            y_re = w_re[:, :pairs] - w_im[:, pairs:]
            y_im = w_re[:, pairs:] + w_im[:, :pairs]
            form_re = jnp.sum(own_re * y_re + own_im * y_im, axis=0, keepdims=True)
            form_im = jnp.sum(own_re * y_im - own_im * y_re, axis=0, keepdims=True)
            out[pl.ds(2 * node, 1), :] = form_re
            out[pl.ds(2 * node + 1, 1), :] = form_im


def add_blocks(y, place, numbers, w_own, w_other, pieces, own=None):
    blocks = len(numbers)
    first, last = y is None, own is not None
    rows, columns = 2 * w_own.shape[0], pieces[0].shape[0] // 2
    width = 4 * pieces[0].shape[1]
    vmem = pl.BlockSpec(memory_space=pltpu.VMEM)
    hbm = pl.BlockSpec(memory_space=pltpu.HBM)
    operands = [place, w_own, w_other, *pieces]
    specs = [pl.BlockSpec(memory_space=pltpu.SMEM), hbm, hbm, *[vmem] * len(pieces)]
    aliases = {}
    if not first:
        if not last:
            aliases = {len(operands): 0}
        operands.append(y)
        specs.append(vmem)
    if last:
        operands.append(own)
        specs.append(vmem)
        shape = (rows // own.shape[1], columns // 2)
    else:
        shape = (rows, columns)
    scratch = [
        pltpu.VMEM((blocks, rows, width), w_own.dtype),
        pltpu.VMEM((blocks, columns, width), pieces[0].dtype),
        pltpu.SemaphoreType.DMA((blocks, 2)),
    ]
    if last:
        scratch.append(pltpu.VMEM((rows, columns), F32))
    return pl.pallas_call(
        functools.partial(block_products, numbers=numbers, first=first, last=last),
        out_shape=jax.ShapeDtypeStruct(shape, F32),
        in_specs=specs,
        out_specs=vmem,
        scratch_shapes=scratch,
        input_output_aliases=aliases,
        compiler_params=pltpu.CompilerParams(vmem_limit_bytes=20 * 2**20),
        cost_estimate=pl.CostEstimate(
            flops=2 * blocks * rows * columns * width,
            bytes_accessed=2 * blocks * rows * width,
            transcendentals=0,
        ),
        name="block_products",
    )(*operands)


def node_factor(node_freq, node_weight, band_energy, energy_grid, pair_band):
    band_onehot = (
        pair_band[:, None] == jnp.arange(band_energy.shape[0], dtype=jnp.int32)[None, :]
    ).astype(F32)
    pair_eps = jnp.dot(band_onehot, band_energy, precision=lax.Precision.HIGHEST)
    delta = energy_grid[None, :] - pair_eps[:, None]
    return (
        node_weight[:, None, None]
        * delta[None]
        / (delta[None] ** 2 + node_freq[:, None, None] ** 2)
    )


def per_device(
    screened, elements, node_freq, node_weight, band_energy, energy_grid, pair_state, pair_band
):
    nodes, _, depth, waves = screened.shape
    npair = elements.shape[1]
    half = npair // lax.axis_size("freq")
    core = lax.axis_index("freq")
    z, x = lax.axis_index("row_0"), lax.axis_index("row_1")
    nz, nx = lax.axis_size("row_0"), lax.axis_size("row_1")

    quadrature = jnp.stack([node_freq, node_weight])
    other_quadrature = shift(quadrature, "freq", 1)
    screened, other_quadrature = lax.optimization_barrier((screened, other_quadrature))
    quadrature = jnp.concatenate([quadrature, other_quadrature], axis=1)
    w_own = screened.reshape(nodes * 2 * depth, waves)
    w_other = shift(w_own, "freq", 1)
    w_own = pltpu.with_memory_space_constraint(w_own, pltpu.HBM)
    w_other = pltpu.with_memory_space_constraint(w_other, pltpu.HBM)

    mine = lax.dynamic_slice_in_dim(elements, core * half, half, 1)
    piece = mine.reshape(2 * half, depth)
    before = shift(piece, "row_1", 1)
    after = shift(piece, "row_1", -1)
    across = shift(piece, "row_1", 2)
    steps = jnp.arange(nz + 4, dtype=jnp.int32)
    along_x = (x + jnp.where(steps == nz + 1, nx - 1, jnp.where(steps == nz, 0, steps - nz - 1))) % nx
    place = jnp.where(steps < nz, (z + steps) % nz, along_x)

    my_band = lax.dynamic_slice_in_dim(pair_band, core * half, half, 0)
    my_state = lax.dynamic_slice_in_dim(pair_state, core * half, half, 0)
    factor = node_factor(quadrature[0], quadrature[1], band_energy, energy_grid, my_band)
    state_onehot = (
        jnp.arange(NSTATE, dtype=jnp.int32)[:, None] == my_state[None, :]
    ).astype(F32)

    far = nz // 2
    up = [jnp.concatenate([piece, before]), jnp.concatenate([after, across])]
    down = list(up)
    numbers, pieces, y = [0], list(up), None
    for r in range(1, far):
        up = [shift(v, "row_0", 1) for v in up]
        down = [shift(v, "row_0", -1) for v in down]
        if r > 1:
            y = add_blocks(y, place, tuple(numbers), w_own, w_other, pieces)
            up[0], down[0], y = lax.optimization_barrier((up[0], down[0], y))
            numbers, pieces = [], []
        if r == 3:
            up[1], down[1], factor, state_onehot = lax.optimization_barrier(
                (up[1], down[1], factor, state_onehot)
            )
        numbers += [nz - r, r]
        pieces += [*up, *down]
    opposite = [shift(up[0], "row_0", 1), shift(down[1], "row_0", -1)]
    y = add_blocks(y, place, tuple(numbers), w_own, w_other, pieces)
    form = add_blocks(y, place, (far,), w_own, w_other, opposite, piece)

    form = sum_over(sum_over(form, "row_1"), "row_0")
    form = form.reshape(2 * nodes, 2, half)

    terms = jnp.sum(form[:, :, :, None] * factor[:, None], axis=0)
    sigma = [jnp.dot(state_onehot, t, precision=lax.Precision.HIGHEST) for t in terms]
    return lax.psum(jnp.stack(sigma), "freq")


def solution(mesh):
    split = Mesh(
        mesh.devices.reshape(mesh.shape["kpt"], 16, 4, mesh.shape["freq"]),
        ("kpt", "row_0", "row_1", "freq"),
    )
    return jax.shard_map(
        per_device,
        mesh=split,
        in_specs=(
            P(("kpt", "freq"), None, ROW, None),
            P(None, "kpt", ROW),
            P("freq"),
            P("freq"),
            P("kpt"),
            P(),
            P("kpt"),
            P("kpt"),
        ),
        out_specs=P(None, "kpt", None),
        check_vma=False,
    )
```

```python
import functools

import jax
import jax.numpy as jnp
from jax import lax
from jax.experimental import pallas as pl
from jax.experimental.pallas import tpu as pltpu
from jax.sharding import Mesh
from jax.sharding import PartitionSpec as P

NSTATE = 32
ROW = ("row_0", "row_1")
F32 = jnp.float32
VMEM_LIMIT = 20 * 2**20


def shift(value, axis, step):
    size = lax.axis_size(axis)
    return lax.ppermute(value, axis, [(i, (i + step) % size) for i in range(size)])


def sum_over(value, axis):
    copies = jnp.broadcast_to(value, (lax.axis_size(axis), *value.shape))
    return lax.all_to_all(copies, axis, split_axis=0, concat_axis=0, tiled=True).sum(axis=0)


def block_products(place, w_own, w_other, *refs, numbers, after, first, last):
    blocks = len(numbers)
    pieces = refs[: 2 * blocks]
    refs = refs[2 * blocks :]
    if not first:
        y_in, w_now, refs = refs[0], refs[1], refs[2:]
    if last:
        own, out, m_buf, y = refs
    elif first:
        y, w_next, m_buf, sems, w_now, first_sems = refs
    else:
        y, w_next, m_buf, sems = refs
    rows, width = w_own.shape[0], m_buf.shape[2]
    columns, lanes = m_buf.shape[1], pieces[0].shape[1]

    def reads(target, wanted, semaphores):
        return [
            pltpu.make_async_copy(
                w.at[:, pl.ds(pl.multiple_of(place[number] * width, width), width)],
                target.at[2 * b + half],
                semaphores.at[2 * b + half],
            )
            for b, number in enumerate(wanted)
            for half, w in enumerate((w_own, w_other))
        ]

    now = reads(w_now, numbers, first_sems) if first else []
    ahead = [] if last else reads(w_next, after, sems)
    for copy in now + ahead:
        copy.start()
    for b in range(blocks):
        for k in range(4):
            lane = pl.multiple_of(place[place.shape[0] - 4 + k] * lanes, lanes)
            piece = pieces[2 * b + k // 2]
            m_buf[b, :, pl.ds(lane, lanes)] = piece[pl.ds((k % 2) * columns, columns), :]
    if last:
        flat = own[...].astype(F32).T
        pairs, depth = columns // 2, own.shape[1]
        own_re, own_im = flat[:, :pairs], flat[:, pairs:]
    for copy in now:
        copy.wait()

    @pl.loop(0, 2)
    def _(half):
        spot = pl.ds(pl.multiple_of(half * rows, rows), rows)
        total = None if first else y_in[spot, :]
        for b in range(blocks):
            term = lax.dot_general(
                w_now[2 * b + half],
                m_buf[b],
                (((1,), (1,)), ((), ())),
                preferred_element_type=F32,
            )
            total = term if total is None else total + term
        y[spot, :] = total

    if last:

        @pl.loop(0, out.shape[0] // 2)
        def _(node):
            base = pl.multiple_of(node * 2 * depth, 2 * depth)
            w_re = y[pl.ds(base, depth), :]
            w_im = y[pl.ds(base + depth, depth), :]
            y_re = w_re[:, :pairs] - w_im[:, pairs:]
            y_im = w_re[:, pairs:] + w_im[:, :pairs]
            form_re = jnp.sum(own_re * y_re + own_im * y_im, axis=0, keepdims=True)
            form_im = jnp.sum(own_re * y_im - own_im * y_re, axis=0, keepdims=True)
            out[pl.ds(2 * node, 1), :] = form_re
            out[pl.ds(2 * node + 1, 1), :] = form_im

    for copy in ahead:
        copy.wait()


def add_blocks(state, place, numbers, after, w_own, w_other, pieces, own=None):
    blocks = len(numbers)
    first, last = state is None, own is not None
    half, columns, width = w_own.shape[0], pieces[0].shape[0] // 2, 4 * pieces[0].shape[1]
    vmem = pl.BlockSpec(memory_space=pltpu.VMEM)
    hbm = pl.BlockSpec(memory_space=pltpu.HBM)
    operands = [place, w_own, w_other, *pieces]
    specs = [pl.BlockSpec(memory_space=pltpu.SMEM), hbm, hbm, *[vmem] * len(pieces)]
    aliases = {}
    if not first:
        if not last:
            aliases = {len(operands): 0}
        operands += state
        specs += [vmem, vmem]
    scratch = [pltpu.VMEM((blocks, columns, width), pieces[0].dtype)]
    if last:
        operands.append(own)
        specs.append(vmem)
        out_shape = jax.ShapeDtypeStruct((2 * half // own.shape[1], columns // 2), F32)
        out_specs = vmem
        scratch.append(pltpu.VMEM((2 * half, columns), F32))
    else:
        out_shape = (
            jax.ShapeDtypeStruct((2 * half, columns), F32),
            jax.ShapeDtypeStruct((2 * len(after), half, width), w_own.dtype),
        )
        out_specs = (vmem, vmem)
        scratch.append(pltpu.SemaphoreType.DMA((2 * len(after),)))
        if first:
            scratch.append(pltpu.VMEM((2 * blocks, half, width), w_own.dtype))
            scratch.append(pltpu.SemaphoreType.DMA((2 * blocks,)))
    return pl.pallas_call(
        functools.partial(
            block_products, numbers=numbers, after=after, first=first, last=last
        ),
        out_shape=out_shape,
        in_specs=specs,
        out_specs=out_specs,
        scratch_shapes=scratch,
        input_output_aliases=aliases,
        compiler_params=pltpu.CompilerParams(vmem_limit_bytes=VMEM_LIMIT),
        cost_estimate=pl.CostEstimate(
            flops=4 * blocks * half * columns * width,
            bytes_accessed=4 * blocks * half * width,
            transcendentals=0,
        ),
        name="block_products",
    )(*operands)


def node_factor(node_freq, node_weight, band_energy, energy_grid, pair_band):
    band_onehot = (
        pair_band[:, None] == jnp.arange(band_energy.shape[0], dtype=jnp.int32)[None, :]
    ).astype(F32)
    pair_eps = jnp.dot(band_onehot, band_energy, precision=lax.Precision.HIGHEST)
    delta = energy_grid[None, :] - pair_eps[:, None]
    return (
        node_weight[:, None, None]
        * delta[None]
        / (delta[None] ** 2 + node_freq[:, None, None] ** 2)
    )


def per_device(
    screened, elements, node_freq, node_weight, band_energy, energy_grid, pair_state, pair_band
):
    nodes, _, depth, waves = screened.shape
    npair = elements.shape[1]
    half = npair // lax.axis_size("freq")
    core = lax.axis_index("freq")
    z, x = lax.axis_index("row_0"), lax.axis_index("row_1")
    nz, nx = lax.axis_size("row_0"), lax.axis_size("row_1")

    quadrature = jnp.stack([node_freq, node_weight])
    other_quadrature = shift(quadrature, "freq", 1)
    screened, other_quadrature = lax.optimization_barrier((screened, other_quadrature))
    quadrature = jnp.concatenate([quadrature, other_quadrature], axis=1)
    w_own = screened.reshape(nodes * 2 * depth, waves)
    w_other = shift(w_own, "freq", 1)
    w_own = pltpu.with_memory_space_constraint(w_own, pltpu.HBM)
    w_other = pltpu.with_memory_space_constraint(w_other, pltpu.HBM)

    mine = lax.dynamic_slice_in_dim(elements, core * half, half, 1)
    piece = mine.reshape(2 * half, depth)
    before = shift(piece, "row_1", 1)
    after = shift(piece, "row_1", -1)
    onward, before = lax.optimization_barrier((piece, before))
    across = shift(onward, "row_1", 2)
    steps = jnp.arange(nz + 4, dtype=jnp.int32)
    along_x = (x + jnp.where(steps == nz + 1, nx - 1, jnp.where(steps == nz, 0, steps - nz - 1))) % nx
    place = jnp.where(steps < nz, (z + steps) % nz, along_x)

    far = nz // 2
    up = [jnp.concatenate([piece, before]), jnp.concatenate([after, across])]
    down = list(up)
    numbers, pieces, state = (0,), list(up), None
    for r in range(1, far):
        up = [shift(v, "row_0", 1) for v in up]
        down = [shift(v, "row_0", -1) for v in down]
        if r > 1:
            state = add_blocks(state, place, numbers, (nz - r, r), w_own, w_other, pieces)
            up[0], down[0], state = lax.optimization_barrier((up[0], down[0], state))
            numbers, pieces = (), []
        if r == 3:
            up[1], down[1], pair_band, pair_state = lax.optimization_barrier(
                (up[1], down[1], pair_band, pair_state)
            )
            my_band = lax.dynamic_slice_in_dim(pair_band, core * half, half, 0)
            my_state = lax.dynamic_slice_in_dim(pair_state, core * half, half, 0)
            factor = node_factor(
                quadrature[0], quadrature[1], band_energy, energy_grid, my_band
            )
            state_onehot = (
                jnp.arange(NSTATE, dtype=jnp.int32)[:, None] == my_state[None, :]
            ).astype(F32)
        if r == 6:
            up[1], down[1], factor, state_onehot = lax.optimization_barrier(
                (up[1], down[1], factor, state_onehot)
            )
        numbers += (nz - r, r)
        pieces += [*up, *down]
    opposite = [shift(up[0], "row_0", 1), shift(down[1], "row_0", -1)]
    state = add_blocks(state, place, numbers, (far,), w_own, w_other, pieces)
    form = add_blocks(state, place, (far,), (), w_own, w_other, opposite, piece)

    form = sum_over(sum_over(form, "row_1"), "row_0")
    form = form.reshape(2 * nodes, 2, half)

    terms = jnp.sum(form[:, :, :, None] * factor[:, None], axis=0)
    sigma = [jnp.dot(state_onehot, t, precision=lax.Precision.HIGHEST) for t in terms]
    return lax.psum(jnp.stack(sigma), "freq")


def solution(mesh):
    split = Mesh(
        mesh.devices.reshape(mesh.shape["kpt"], 16, 4, mesh.shape["freq"]),
        ("kpt", "row_0", "row_1", "freq"),
    )
    return jax.shard_map(
        per_device,
        mesh=split,
        in_specs=(
            P(("kpt", "freq"), None, ROW, None),
            P(None, "kpt", ROW),
            P("freq"),
            P("freq"),
            P("kpt"),
            P(),
            P("kpt"),
            P("kpt"),
        ),
        out_specs=P(None, "kpt", None),
        check_vma=False,
    )
```

```python
import functools

import jax
import jax.numpy as jnp
from jax import lax
from jax.experimental import pallas as pl
from jax.experimental.pallas import tpu as pltpu
from jax.sharding import Mesh
from jax.sharding import PartitionSpec as P

NSTATE = 32
ROW = ("row_0", "row_1")
F32 = jnp.float32
VMEM_LIMIT = 20 * 2**20


def shift(value, axis, step):
    size = lax.axis_size(axis)
    return lax.ppermute(value, axis, [(i, (i + step) % size) for i in range(size)])


def sum_over(value, axis):
    copies = jnp.broadcast_to(value, (lax.axis_size(axis), *value.shape))
    return lax.all_to_all(copies, axis, split_axis=0, concat_axis=0, tiled=True).sum(axis=0)


def block_products(place, w_own, w_other, *refs, numbers, after, first, last):
    blocks = len(numbers)
    pieces = refs[: 2 * blocks]
    refs = refs[2 * blocks :]
    if not first:
        y_in, w_now, refs = refs[0], refs[1], refs[2:]
    if last:
        own, out, m_buf, y = refs
    elif first:
        y, w_next, m_buf, sems, w_now, first_sems = refs
    else:
        y, w_next, m_buf, sems = refs
    rows, width = w_own.shape[0], m_buf.shape[2]
    columns, lanes = m_buf.shape[1], pieces[0].shape[1]

    def reads(target, wanted, semaphores):
        return [
            pltpu.make_async_copy(
                w.at[:, pl.ds(pl.multiple_of(place[number] * width, width), width)],
                target.at[2 * b + half],
                semaphores.at[2 * b + half],
            )
            for b, number in enumerate(wanted)
            for half, w in enumerate((w_own, w_other))
        ]

    now = reads(w_now, numbers, first_sems) if first else []
    ahead = [] if last else reads(w_next, after, sems)
    for copy in now + ahead:
        copy.start()
    for b in range(blocks):
        for k in range(4):
            lane = pl.multiple_of(place[place.shape[0] - 4 + k] * lanes, lanes)
            piece = pieces[2 * b + k // 2]
            m_buf[b, :, pl.ds(lane, lanes)] = piece[pl.ds((k % 2) * columns, columns), :]
    if last:
        flat = own[...].astype(F32).T
        pairs, depth = columns // 2, own.shape[1]
        own_re, own_im = flat[:, :pairs], flat[:, pairs:]
    for copy in now:
        copy.wait()

    @pl.loop(0, 2)
    def _(half):
        spot = pl.ds(pl.multiple_of(half * rows, rows), rows)
        total = None if first else y_in[spot, :]
        for b in range(blocks):
            term = lax.dot_general(
                w_now[2 * b + half],
                m_buf[b],
                (((1,), (1,)), ((), ())),
                preferred_element_type=F32,
            )
            total = term if total is None else total + term
        y[spot, :] = total

    if last:

        @pl.loop(0, out.shape[0] // 2)
        def _(node):
            base = pl.multiple_of(node * 2 * depth, 2 * depth)
            w_re = y[pl.ds(base, depth), :]
            w_im = y[pl.ds(base + depth, depth), :]
            y_re = w_re[:, :pairs] - w_im[:, pairs:]
            y_im = w_re[:, pairs:] + w_im[:, :pairs]
            form_re = jnp.sum(own_re * y_re + own_im * y_im, axis=0, keepdims=True)
            form_im = jnp.sum(own_re * y_im - own_im * y_re, axis=0, keepdims=True)
            out[pl.ds(2 * node, 1), :] = form_re
            out[pl.ds(2 * node + 1, 1), :] = form_im

    for copy in ahead:
        copy.wait()


def add_blocks(state, place, numbers, after, w_own, w_other, pieces, own=None):
    blocks = len(numbers)
    first, last = state is None, own is not None
    half, columns, width = w_own.shape[0], pieces[0].shape[0] // 2, 4 * pieces[0].shape[1]
    vmem = pl.BlockSpec(memory_space=pltpu.VMEM)
    hbm = pl.BlockSpec(memory_space=pltpu.HBM)
    operands = [place, w_own, w_other, *pieces]
    specs = [pl.BlockSpec(memory_space=pltpu.SMEM), hbm, hbm, *[vmem] * len(pieces)]
    aliases = {}
    if not first:
        if not last:
            aliases = {len(operands): 0}
        operands += state
        specs += [vmem, vmem]
    scratch = [pltpu.VMEM((blocks, columns, width), pieces[0].dtype)]
    if last:
        operands.append(own)
        specs.append(vmem)
        out_shape = jax.ShapeDtypeStruct((2 * half // own.shape[1], columns // 2), F32)
        out_specs = vmem
        scratch.append(pltpu.VMEM((2 * half, columns), F32))
    else:
        out_shape = (
            jax.ShapeDtypeStruct((2 * half, columns), F32),
            jax.ShapeDtypeStruct((2 * len(after), half, width), w_own.dtype),
        )
        out_specs = (vmem, vmem)
        scratch.append(pltpu.SemaphoreType.DMA((2 * len(after),)))
        if first:
            scratch.append(pltpu.VMEM((2 * blocks, half, width), w_own.dtype))
            scratch.append(pltpu.SemaphoreType.DMA((2 * blocks,)))
    return pl.pallas_call(
        functools.partial(
            block_products, numbers=numbers, after=after, first=first, last=last
        ),
        out_shape=out_shape,
        in_specs=specs,
        out_specs=out_specs,
        scratch_shapes=scratch,
        input_output_aliases=aliases,
        compiler_params=pltpu.CompilerParams(vmem_limit_bytes=VMEM_LIMIT),
        cost_estimate=pl.CostEstimate(
            flops=4 * blocks * half * columns * width,
            bytes_accessed=4 * blocks * half * width,
            transcendentals=0,
        ),
        name="block_products",
    )(*operands)


def node_factor(node_freq, node_weight, band_energy, energy_grid, pair_band):
    band_onehot = (
        pair_band[:, None] == jnp.arange(band_energy.shape[0], dtype=jnp.int32)[None, :]
    ).astype(F32)
    pair_eps = jnp.dot(band_onehot, band_energy, precision=lax.Precision.HIGHEST)
    delta = energy_grid[None, :] - pair_eps[:, None]
    return (
        node_weight[:, None, None]
        * delta[None]
        / (delta[None] ** 2 + node_freq[:, None, None] ** 2)
    )


def per_device(
    screened, elements, node_freq, node_weight, band_energy, energy_grid, pair_state, pair_band
):
    nodes, _, depth, waves = screened.shape
    npair = elements.shape[1]
    half = npair // lax.axis_size("freq")
    core = lax.axis_index("freq")
    z, x = lax.axis_index("row_0"), lax.axis_index("row_1")
    nz, nx = lax.axis_size("row_0"), lax.axis_size("row_1")

    quadrature = jnp.stack([node_freq, node_weight])
    other_quadrature = shift(quadrature, "freq", 1)
    screened, other_quadrature = lax.optimization_barrier((screened, other_quadrature))
    quadrature = jnp.concatenate([quadrature, other_quadrature], axis=1)
    w_own = screened.reshape(nodes * 2 * depth, waves)
    w_other = shift(w_own, "freq", 1)
    w_own = pltpu.with_memory_space_constraint(w_own, pltpu.HBM)
    w_other = pltpu.with_memory_space_constraint(w_other, pltpu.HBM)

    mine = lax.dynamic_slice_in_dim(elements, core * half, half, 1)
    piece = mine.reshape(2 * half, depth)
    before = shift(piece, "row_1", 1)
    after = shift(piece, "row_1", -1)
    across = shift(piece, "row_1", 2)
    steps = jnp.arange(nz + 4, dtype=jnp.int32)
    along_x = (x + jnp.where(steps == nz + 1, nx - 1, jnp.where(steps == nz, 0, steps - nz - 1))) % nx
    place = jnp.where(steps < nz, (z + steps) % nz, along_x)

    my_band = lax.dynamic_slice_in_dim(pair_band, core * half, half, 0)
    my_state = lax.dynamic_slice_in_dim(pair_state, core * half, half, 0)
    factor = node_factor(
        quadrature[0], quadrature[1], band_energy, energy_grid, my_band
    )
    state_onehot = (
        jnp.arange(NSTATE, dtype=jnp.int32)[:, None] == my_state[None, :]
    ).astype(F32)

    far = nz // 2
    up = [jnp.concatenate([piece, before]), jnp.concatenate([after, across])]
    down = list(up)
    numbers, pieces, state = (0,), list(up), None
    for r in range(1, far):
        up = [shift(v, "row_0", 1) for v in up]
        down = [shift(v, "row_0", -1) for v in down]
        if r > 1:
            state = add_blocks(state, place, numbers, (nz - r, r), w_own, w_other, pieces)
            up[0], down[0], state = lax.optimization_barrier((up[0], down[0], state))
            numbers, pieces = (), []
        if r == 3:
            up[1], down[1], factor, state_onehot = lax.optimization_barrier(
                (up[1], down[1], factor, state_onehot)
            )
        numbers += (nz - r, r)
        pieces += [*up, *down]
    opposite = [shift(up[0], "row_0", 1), shift(down[1], "row_0", -1)]
    state = add_blocks(state, place, numbers, (far,), w_own, w_other, pieces)
    form = add_blocks(state, place, (far,), (), w_own, w_other, opposite, piece)

    form = sum_over(sum_over(form, "row_1"), "row_0")
    form = form.reshape(2 * nodes, 2, half)

    terms = jnp.sum(form[:, :, :, None] * factor[:, None], axis=0)
    sigma = [jnp.dot(state_onehot, t, precision=lax.Precision.HIGHEST) for t in terms]
    return lax.psum(jnp.stack(sigma), "freq")


def solution(mesh):
    split = Mesh(
        mesh.devices.reshape(mesh.shape["kpt"], 16, 4, mesh.shape["freq"]),
        ("kpt", "row_0", "row_1", "freq"),
    )
    return jax.shard_map(
        per_device,
        mesh=split,
        in_specs=(
            P(("kpt", "freq"), None, ROW, None),
            P(None, "kpt", ROW),
            P("freq"),
            P("freq"),
            P("kpt"),
            P(),
            P("kpt"),
            P("kpt"),
        ),
        out_specs=P(None, "kpt", None),
        check_vma=False,
    )
```

```python
import functools

import jax
import jax.numpy as jnp
from jax import lax
from jax.experimental import pallas as pl
from jax.experimental.pallas import tpu as pltpu
from jax.sharding import Mesh
from jax.sharding import PartitionSpec as P

NSTATE = 32
ROW = ("row_0", "row_1")
F32 = jnp.float32
VMEM_LIMIT = 20 * 2**20


def shift(value, axis, step):
    size = lax.axis_size(axis)
    return lax.ppermute(value, axis, [(i, (i + step) % size) for i in range(size)])


def block_products(place, w_own, w_other, *refs, numbers, after, first, last):
    blocks = len(numbers)
    pieces = refs[: 2 * blocks]
    refs = refs[2 * blocks :]
    if not first:
        y_in, w_now, refs = refs[0], refs[1], refs[2:]
    if last:
        own, out, m_buf, y = refs
    elif first:
        y, w_next, m_buf, sems, w_now, first_sems = refs
    else:
        y, w_next, m_buf, sems = refs
    rows, width = w_own.shape[0], m_buf.shape[2]
    columns, lanes = m_buf.shape[1], pieces[0].shape[1]

    def reads(target, wanted, semaphores):
        return [
            pltpu.make_async_copy(
                w.at[:, pl.ds(pl.multiple_of(place[number] * width, width), width)],
                target.at[2 * b + half],
                semaphores.at[2 * b + half],
            )
            for b, number in enumerate(wanted)
            for half, w in enumerate((w_own, w_other))
        ]

    now = reads(w_now, numbers, first_sems) if first else []
    ahead = [] if last else reads(w_next, after, sems)
    for copy in now + ahead:
        copy.start()
    for b in range(blocks):
        for k in range(4):
            lane = pl.multiple_of(place[place.shape[0] - 4 + k] * lanes, lanes)
            piece = pieces[2 * b + k // 2]
            m_buf[b, :, pl.ds(lane, lanes)] = piece[pl.ds((k % 2) * columns, columns), :]
    if last:
        flat = own[...].astype(F32).T
        pairs, depth = columns // 2, own.shape[1]
        own_re, own_im = flat[:, :pairs], flat[:, pairs:]
    for copy in now:
        copy.wait()

    @pl.loop(0, 2)
    def _(half):
        spot = pl.ds(pl.multiple_of(half * rows, rows), rows)
        total = None if first else y_in[spot, :]
        for b in range(blocks):
            term = lax.dot_general(
                w_now[2 * b + half],
                m_buf[b],
                (((1,), (1,)), ((), ())),
                preferred_element_type=F32,
            )
            total = term if total is None else total + term
        y[spot, :] = total

    if last:

        @pl.loop(0, out.shape[0] // 2)
        def _(node):
            base = pl.multiple_of(node * 2 * depth, 2 * depth)
            w_re = y[pl.ds(base, depth), :]
            w_im = y[pl.ds(base + depth, depth), :]
            y_re = w_re[:, :pairs] - w_im[:, pairs:]
            y_im = w_re[:, pairs:] + w_im[:, :pairs]
            form_re = jnp.sum(own_re * y_re + own_im * y_im, axis=0, keepdims=True)
            form_im = jnp.sum(own_re * y_im - own_im * y_re, axis=0, keepdims=True)
            out[pl.ds(2 * node, 1), :] = form_re
            out[pl.ds(2 * node + 1, 1), :] = form_im

    for copy in ahead:
        copy.wait()


def add_blocks(state, place, numbers, after, w_own, w_other, pieces, own=None):
    blocks = len(numbers)
    first, last = state is None, own is not None
    half, columns, width = w_own.shape[0], pieces[0].shape[0] // 2, 4 * pieces[0].shape[1]
    vmem = pl.BlockSpec(memory_space=pltpu.VMEM)
    hbm = pl.BlockSpec(memory_space=pltpu.HBM)
    operands = [place, w_own, w_other, *pieces]
    specs = [pl.BlockSpec(memory_space=pltpu.SMEM), hbm, hbm, *[vmem] * len(pieces)]
    aliases = {}
    if not first:
        if not last:
            aliases = {len(operands): 0}
        operands += state
        specs += [vmem, vmem]
    scratch = [pltpu.VMEM((blocks, columns, width), pieces[0].dtype)]
    if last:
        operands.append(own)
        specs.append(vmem)
        out_shape = jax.ShapeDtypeStruct((2 * half // own.shape[1], columns // 2), F32)
        out_specs = vmem
        scratch.append(pltpu.VMEM((2 * half, columns), F32))
    else:
        out_shape = (
            jax.ShapeDtypeStruct((2 * half, columns), F32),
            jax.ShapeDtypeStruct((2 * len(after), half, width), w_own.dtype),
        )
        out_specs = (vmem, vmem)
        scratch.append(pltpu.SemaphoreType.DMA((2 * len(after),)))
        if first:
            scratch.append(pltpu.VMEM((2 * blocks, half, width), w_own.dtype))
            scratch.append(pltpu.SemaphoreType.DMA((2 * blocks,)))
    return pl.pallas_call(
        functools.partial(
            block_products, numbers=numbers, after=after, first=first, last=last
        ),
        out_shape=out_shape,
        in_specs=specs,
        out_specs=out_specs,
        scratch_shapes=scratch,
        input_output_aliases=aliases,
        compiler_params=pltpu.CompilerParams(vmem_limit_bytes=VMEM_LIMIT),
        cost_estimate=pl.CostEstimate(
            flops=4 * blocks * half * columns * width,
            bytes_accessed=4 * blocks * half * width,
            transcendentals=0,
        ),
        name="block_products",
    )(*operands)


def node_factor(node_freq, node_weight, band_energy, energy_grid, pair_band):
    band_onehot = (
        pair_band[:, None] == jnp.arange(band_energy.shape[0], dtype=jnp.int32)[None, :]
    ).astype(F32)
    pair_eps = jnp.dot(band_onehot, band_energy, precision=lax.Precision.HIGHEST)
    delta = energy_grid[:, None] - pair_eps[None, :]
    return (
        node_weight[:, None, None]
        * delta[None]
        / (delta[None] ** 2 + node_freq[:, None, None] ** 2)
    )


def states_kernel(forms, factor, onehot, out):
    nodes, pairs = factor.shape[0], forms.shape[2]
    halves = factor.shape[2] // pairs
    form = jnp.sum(forms[...], axis=0)
    for part in range(2):
        total = None
        for h in range(halves):
            spot = pl.ds(h * pairs, pairs)
            row = 2 * nodes * h + part
            terms = form[row : row + 1, :] * factor[0, :, spot]
            for node in range(1, nodes):
                row = 2 * (nodes * h + node) + part
                terms += form[row : row + 1, :] * factor[node, :, spot]
            term = lax.dot_general(
                onehot[:, spot],
                terms,
                (((1,), (1,)), ((), ())),
                precision=lax.Precision.HIGHEST,
                preferred_element_type=F32,
            )
            total = term if total is None else total + term
        out[part] = total


def per_state(forms, factor, onehot):
    vmem = pl.BlockSpec(memory_space=pltpu.VMEM)
    return pl.pallas_call(
        states_kernel,
        out_shape=jax.ShapeDtypeStruct((2, onehot.shape[0], factor.shape[1]), F32),
        in_specs=[vmem] * 3,
        out_specs=vmem,
        compiler_params=pltpu.CompilerParams(vmem_limit_bytes=VMEM_LIMIT),
        name="per_state",
    )(forms, factor, onehot)


def per_device(
    screened, elements, node_freq, node_weight, band_energy, energy_grid, pair_state, pair_band
):
    nodes, _, depth, waves = screened.shape
    npair = elements.shape[1]
    half = npair // lax.axis_size("freq")
    core = lax.axis_index("freq")
    z, x = lax.axis_index("row_0"), lax.axis_index("row_1")
    nz, nx = lax.axis_size("row_0"), lax.axis_size("row_1")

    w_own = screened.reshape(nodes * 2 * depth, waves)
    w_other = shift(w_own, "freq", 1)
    w_own = pltpu.with_memory_space_constraint(w_own, pltpu.HBM)
    w_other = pltpu.with_memory_space_constraint(w_other, pltpu.HBM)

    mine = lax.dynamic_slice_in_dim(elements, core * half, half, 1)
    piece = mine.reshape(2 * half, depth)
    before = shift(piece, "row_1", 1)
    after = shift(piece, "row_1", -1)
    across = shift(piece, "row_1", 2)
    steps = jnp.arange(nz + 4, dtype=jnp.int32)
    offset = steps - nz
    offset = jnp.where(offset == 1, nx // 2, jnp.where(offset == 2, nx - 1, offset // 3))
    place = jnp.where(steps < nz, (z + steps) % nz, (x + offset) % nx)

    factor = node_factor(node_freq, node_weight, band_energy, energy_grid, pair_band)
    state_onehot = (
        jnp.arange(NSTATE, dtype=jnp.int32)[:, None] == pair_state[None, :]
    ).astype(F32)

    far = nz // 2
    up = [jnp.concatenate([piece, across]), jnp.concatenate([before, after])]
    down = list(up)
    numbers, pieces, state = (0,), list(up), None
    for r in range(1, far):
        up = [shift(v, "row_0", 1) for v in up]
        down = [shift(v, "row_0", -1) for v in down]
        if r > 1:
            state = add_blocks(state, place, numbers, (nz - r, r), w_own, w_other, pieces)
            up[0], down[0], state = lax.optimization_barrier((up[0], down[0], state))
            numbers, pieces = (), []
        if r == 3:
            up[1], down[1], factor, state_onehot = lax.optimization_barrier(
                (up[1], down[1], factor, state_onehot)
            )
        numbers += (nz - r, r)
        pieces += [*up, *down]
    opposite = [shift(up[0], "row_0", 1), shift(down[1], "row_0", -1)]
    state = add_blocks(state, place, numbers, (far,), w_own, w_other, pieces)
    form = add_blocks(state, place, (far,), (), w_own, w_other, opposite, piece)

    kept, given = form[: 2 * nodes], form[2 * nodes :]
    sent = jnp.stack([jnp.where(core == 0, kept, given), jnp.where(core == 0, given, kept)])
    sent = jnp.broadcast_to(sent, (nx, *sent.shape)).reshape(-1, *kept.shape)
    form = lax.all_to_all(sent, ("row_1", "freq"), split_axis=0, concat_axis=0, tiled=True)
    form = form.reshape(nx, -1, half).sum(axis=0)
    forms = lax.all_to_all(
        jnp.broadcast_to(form, (nz, *form.shape)), "row_0", split_axis=0, concat_axis=0, tiled=True
    )
    sigma = per_state(forms, factor, state_onehot)
    return sigma + shift(sigma, "freq", 1)


def solution(mesh):
    split = Mesh(
        mesh.devices.reshape(mesh.shape["kpt"], 16, 4, mesh.shape["freq"]),
        ("kpt", "row_0", "row_1", "freq"),
    )
    return jax.shard_map(
        per_device,
        mesh=split,
        in_specs=(
            P(("kpt", "freq"), None, ROW, None),
            P(None, "kpt", ROW),
            P("freq"),
            P("freq"),
            P("kpt"),
            P(),
            P("kpt"),
            P("kpt"),
        ),
        out_specs=P(None, "kpt", None),
        check_vma=False,
    )
```

```python
import functools

import jax
import jax.numpy as jnp
from jax import lax
from jax.experimental import pallas as pl
from jax.experimental.pallas import tpu as pltpu
from jax.sharding import Mesh
from jax.sharding import PartitionSpec as P

NSTATE = 32
ROW = ("row_0", "row_1")
F32 = jnp.float32
VMEM_LIMIT = 20 * 2**20


def shift(value, axis, step):
    size = lax.axis_size(axis)
    return lax.ppermute(value, axis, [(i, (i + step) % size) for i in range(size)])


def block_products(place, w_own, w_other, *refs, numbers, after, first, last):
    blocks = len(numbers)
    pieces = refs[: 2 * blocks]
    refs = refs[2 * blocks :]
    if not first:
        y_in, w_now, refs = refs[0], refs[1], refs[2:]
    if last:
        own, out, m_buf, y = refs
    elif first:
        y, w_next, m_buf, sems, w_now, first_sems = refs
    else:
        y, w_next, m_buf, sems = refs
    rows, width = w_own.shape[0], m_buf.shape[2]
    columns, lanes = m_buf.shape[1], pieces[0].shape[1]

    def reads(target, wanted, semaphores):
        return [
            pltpu.make_async_copy(
                w.at[:, pl.ds(pl.multiple_of(place[number] * width, width), width)],
                target.at[2 * b + half],
                semaphores.at[2 * b + half],
            )
            for b, number in enumerate(wanted)
            for half, w in enumerate((w_own, w_other))
        ]

    now = reads(w_now, numbers, first_sems) if first else []
    ahead = [] if last else reads(w_next, after, sems)
    for copy in now + ahead:
        copy.start()
    for b in range(blocks):
        for k in range(4):
            lane = pl.multiple_of(place[place.shape[0] - 5 + k] * lanes, lanes)
            piece = pieces[2 * b + k // 2]
            m_buf[b, :, pl.ds(lane, lanes)] = piece[pl.ds((k % 2) * columns, columns), :]
    if last:
        flat = own[...].astype(F32).T
        pairs, depth = columns // 2, own.shape[1]
        own_re, own_im = flat[:, :pairs], flat[:, pairs:]
    for copy in now:
        copy.wait()

    @pl.loop(0, 2)
    def _(half):
        spot = pl.ds(pl.multiple_of(half * rows, rows), rows)
        total = None if first else y_in[spot, :]
        for b in range(blocks):
            term = lax.dot_general(
                w_now[2 * b + half],
                m_buf[b],
                (((1,), (1,)), ((), ())),
                preferred_element_type=F32,
            )
            total = term if total is None else total + term
        y[spot, :] = total

    if last:
        per_core = out.shape[0] // 4

        @pl.loop(0, out.shape[0] // 2)
        def _(node):
            base = pl.multiple_of(node * 2 * depth, 2 * depth)
            w_re = y[pl.ds(base, depth), :]
            w_im = y[pl.ds(base + depth, depth), :]
            y_re = w_re[:, :pairs] - w_im[:, pairs:]
            y_im = w_re[:, pairs:] + w_im[:, :pairs]
            form_re = jnp.sum(own_re * y_re + own_im * y_im, axis=0, keepdims=True)
            form_im = jnp.sum(own_re * y_im - own_im * y_re, axis=0, keepdims=True)
            half = (node // per_core + place[place.shape[0] - 1]) % 2
            spot = 2 * (half * per_core + node % per_core)
            out[pl.ds(spot, 1), :] = form_re
            out[pl.ds(spot + 1, 1), :] = form_im

    for copy in ahead:
        copy.wait()


def add_blocks(state, place, numbers, after, w_own, w_other, pieces, own=None):
    blocks = len(numbers)
    first, last = state is None, own is not None
    half, columns, width = w_own.shape[0], pieces[0].shape[0] // 2, 4 * pieces[0].shape[1]
    vmem = pl.BlockSpec(memory_space=pltpu.VMEM)
    hbm = pl.BlockSpec(memory_space=pltpu.HBM)
    operands = [place, w_own, w_other, *pieces]
    specs = [pl.BlockSpec(memory_space=pltpu.SMEM), hbm, hbm, *[vmem] * len(pieces)]
    aliases = {}
    if not first:
        if not last:
            aliases = {len(operands): 0}
        operands += state
        specs += [vmem, vmem]
    scratch = [pltpu.VMEM((blocks, columns, width), pieces[0].dtype)]
    if last:
        operands.append(own)
        specs.append(vmem)
        out_shape = jax.ShapeDtypeStruct((2 * half // own.shape[1], columns // 2), F32)
        out_specs = vmem
        scratch.append(pltpu.VMEM((2 * half, columns), F32))
    else:
        out_shape = (
            jax.ShapeDtypeStruct((2 * half, columns), F32),
            jax.ShapeDtypeStruct((2 * len(after), half, width), w_own.dtype),
        )
        out_specs = (vmem, vmem)
        scratch.append(pltpu.SemaphoreType.DMA((2 * len(after),)))
        if first:
            scratch.append(pltpu.VMEM((2 * blocks, half, width), w_own.dtype))
            scratch.append(pltpu.SemaphoreType.DMA((2 * blocks,)))
    return pl.pallas_call(
        functools.partial(
            block_products, numbers=numbers, after=after, first=first, last=last
        ),
        out_shape=out_shape,
        in_specs=specs,
        out_specs=out_specs,
        scratch_shapes=scratch,
        input_output_aliases=aliases,
        compiler_params=pltpu.CompilerParams(vmem_limit_bytes=VMEM_LIMIT),
        cost_estimate=pl.CostEstimate(
            flops=4 * blocks * half * columns * width,
            bytes_accessed=4 * blocks * half * width,
            transcendentals=0,
        ),
        name="block_products",
    )(*operands)


def node_factor(node_freq, node_weight, band_energy, energy_grid, pair_band):
    band_onehot = (
        pair_band[:, None] == jnp.arange(band_energy.shape[0], dtype=jnp.int32)[None, :]
    ).astype(F32)
    pair_eps = jnp.dot(band_onehot, band_energy, precision=lax.Precision.HIGHEST)
    delta = energy_grid[:, None] - pair_eps[None, :]
    return (
        node_weight[:, None, None]
        * delta[None]
        / (delta[None] ** 2 + node_freq[:, None, None] ** 2)
    )


def states_kernel(forms, factor, onehot, out):
    nodes, pairs = factor.shape[0], forms.shape[2]
    halves = factor.shape[2] // pairs
    form = jnp.sum(forms[...], axis=0)
    for part in range(2):
        total = None
        for h in range(halves):
            spot = pl.ds(h * pairs, pairs)
            row = 2 * nodes * h + part
            terms = form[row : row + 1, :] * factor[0, :, spot]
            for node in range(1, nodes):
                row = 2 * (nodes * h + node) + part
                terms += form[row : row + 1, :] * factor[node, :, spot]
            term = lax.dot_general(
                onehot[:, spot],
                terms,
                (((1,), (1,)), ((), ())),
                precision=lax.Precision.HIGHEST,
                preferred_element_type=F32,
            )
            total = term if total is None else total + term
        out[part] = total


def per_state(forms, factor, onehot):
    vmem = pl.BlockSpec(memory_space=pltpu.VMEM)
    return pl.pallas_call(
        states_kernel,
        out_shape=jax.ShapeDtypeStruct((2, onehot.shape[0], factor.shape[1]), F32),
        in_specs=[vmem] * 3,
        out_specs=vmem,
        compiler_params=pltpu.CompilerParams(vmem_limit_bytes=VMEM_LIMIT),
        name="per_state",
    )(forms, factor, onehot)


def per_device(
    screened, elements, node_freq, node_weight, band_energy, energy_grid, pair_state, pair_band
):
    nodes, _, depth, waves = screened.shape
    npair = elements.shape[1]
    half = npair // lax.axis_size("freq")
    core = lax.axis_index("freq")
    z, x = lax.axis_index("row_0"), lax.axis_index("row_1")
    nz, nx = lax.axis_size("row_0"), lax.axis_size("row_1")

    w_own = screened.reshape(nodes * 2 * depth, waves)
    w_other = shift(w_own, "freq", 1)
    w_own = pltpu.with_memory_space_constraint(w_own, pltpu.HBM)
    w_other = pltpu.with_memory_space_constraint(w_other, pltpu.HBM)

    mine = lax.dynamic_slice_in_dim(elements, core * half, half, 1)
    piece = mine.reshape(2 * half, depth)
    before = shift(piece, "row_1", 1)
    after = shift(piece, "row_1", -1)
    across = shift(piece, "row_1", 2)
    steps = jnp.arange(nz + 5, dtype=jnp.int32)
    offset = steps - nz
    offset = jnp.where(offset == 1, nx // 2, jnp.where(offset == 2, nx - 1, offset // 3))
    place = jnp.where(steps < nz, (z + steps) % nz, (x + offset) % nx)
    place = jnp.where(steps == nz + 4, core, place)

    factor = node_factor(node_freq, node_weight, band_energy, energy_grid, pair_band)
    state_onehot = (
        jnp.arange(NSTATE, dtype=jnp.int32)[:, None] == pair_state[None, :]
    ).astype(F32)

    far = nz // 2
    up = [jnp.concatenate([piece, across]), jnp.concatenate([before, after])]
    down = list(up)
    numbers, pieces, state = (0,), list(up), None
    for r in range(1, far):
        up = [shift(v, "row_0", 1) for v in up]
        down = [shift(v, "row_0", -1) for v in down]
        state = add_blocks(state, place, numbers, (nz - r, r), w_own, w_other, pieces)
        up[0], down[0], state = lax.optimization_barrier((up[0], down[0], state))
        numbers, pieces = (), []
        if r == 3:
            up[1], down[1], factor, state_onehot = lax.optimization_barrier(
                (up[1], down[1], factor, state_onehot)
            )
        numbers += (nz - r, r)
        pieces += [*up, *down]
    opposite = [shift(up[0], "row_0", 1), shift(down[1], "row_0", -1)]
    state = add_blocks(state, place, numbers, (far,), w_own, w_other, pieces)
    form = add_blocks(state, place, (far,), (), w_own, w_other, opposite, piece)

    sent = jnp.broadcast_to(form, (nx, *form.shape)).reshape(-1, 2 * nodes, half)
    form = lax.all_to_all(sent, ("row_1", "freq"), split_axis=0, concat_axis=0, tiled=True)
    form = form.reshape(nx, -1, half).sum(axis=0)
    forms = lax.all_to_all(
        jnp.broadcast_to(form, (nz, *form.shape)), "row_0", split_axis=0, concat_axis=0, tiled=True
    )
    sigma = per_state(forms, factor, state_onehot)
    return sigma + shift(sigma, "freq", 1)


def solution(mesh):
    split = Mesh(
        mesh.devices.reshape(mesh.shape["kpt"], 16, 4, mesh.shape["freq"]),
        ("kpt", "row_0", "row_1", "freq"),
    )
    return jax.shard_map(
        per_device,
        mesh=split,
        in_specs=(
            P(("kpt", "freq"), None, ROW, None),
            P(None, "kpt", ROW),
            P("freq"),
            P("freq"),
            P("kpt"),
            P(),
            P("kpt"),
            P("kpt"),
        ),
        out_specs=P(None, "kpt", None),
        check_vma=False,
    )
```

```python
import functools

import jax
import jax.numpy as jnp
from jax import lax
from jax.experimental import pallas as pl
from jax.experimental.pallas import tpu as pltpu
from jax.sharding import Mesh
from jax.sharding import PartitionSpec as P

NSTATE = 32
ROW = ("row_0", "row_1")
F32 = jnp.float32
VMEM_LIMIT = 20 * 2**20


def shift(value, axis, step):
    size = lax.axis_size(axis)
    return lax.ppermute(value, axis, [(i, (i + step) % size) for i in range(size)])


def block_products(place, w_own, w_other, *refs, numbers, after, first, last):
    blocks = len(numbers)
    pieces = refs[: 2 * blocks]
    refs = refs[2 * blocks :]
    if not first:
        y_in, w_now, refs = refs[0], refs[1], refs[2:]
    if last:
        own, out, m_buf, y = refs
    elif first:
        y, w_next, m_buf, sems, w_now, first_sems = refs
    else:
        y, w_next, m_buf, sems = refs
    rows, width = w_own.shape[0], m_buf.shape[2]
    columns, lanes = m_buf.shape[1], pieces[0].shape[1]

    def reads(target, wanted, semaphores):
        return [
            pltpu.make_async_copy(
                w.at[:, pl.ds(pl.multiple_of(place[number] * width, width), width)],
                target.at[2 * b + half],
                semaphores.at[2 * b + half],
            )
            for b, number in enumerate(wanted)
            for half, w in enumerate((w_own, w_other))
        ]

    now = reads(w_now, numbers, first_sems) if first else []
    ahead = [] if last else reads(w_next, after, sems)
    for copy in now + ahead:
        copy.start()
    for b in range(blocks):
        for k in range(4):
            lane = pl.multiple_of(place[place.shape[0] - 5 + k] * lanes, lanes)
            piece = pieces[2 * b + k // 2]
            m_buf[b, :, pl.ds(lane, lanes)] = piece[pl.ds((k % 2) * columns, columns), :]
    if last:
        flat = own[...].astype(F32).T
        pairs, depth = columns // 2, own.shape[1]
        own_re, own_im = flat[:, :pairs], flat[:, pairs:]
    for copy in now:
        copy.wait()

    @pl.loop(0, 2)
    def _(half):
        spot = pl.ds(pl.multiple_of(half * rows, rows), rows)
        total = None if first else y_in[spot, :]
        for b in range(blocks):
            term = lax.dot_general(
                w_now[2 * b + half],
                m_buf[b],
                (((1,), (1,)), ((), ())),
                preferred_element_type=F32,
            )
            total = term if total is None else total + term
        y[spot, :] = total

    if last:
        per_core = out.shape[0] // 4

        @pl.loop(0, out.shape[0] // 2)
        def _(node):
            base = pl.multiple_of(node * 2 * depth, 2 * depth)
            w_re = y[pl.ds(base, depth), :]
            w_im = y[pl.ds(base + depth, depth), :]
            y_re = w_re[:, :pairs] - w_im[:, pairs:]
            y_im = w_re[:, pairs:] + w_im[:, :pairs]
            form_re = jnp.sum(own_re * y_re + own_im * y_im, axis=0, keepdims=True)
            form_im = jnp.sum(own_re * y_im - own_im * y_re, axis=0, keepdims=True)
            half = (node // per_core + place[place.shape[0] - 1]) % 2
            spot = 2 * (half * per_core + node % per_core)
            out[pl.ds(spot, 1), :] = form_re
            out[pl.ds(spot + 1, 1), :] = form_im

    for copy in ahead:
        copy.wait()


def add_blocks(state, place, numbers, after, w_own, w_other, pieces, own=None):
    blocks = len(numbers)
    first, last = state is None, own is not None
    half, columns, width = w_own.shape[0], pieces[0].shape[0] // 2, 4 * pieces[0].shape[1]
    vmem = pl.BlockSpec(memory_space=pltpu.VMEM)
    hbm = pl.BlockSpec(memory_space=pltpu.HBM)
    operands = [place, w_own, w_other, *pieces]
    specs = [pl.BlockSpec(memory_space=pltpu.SMEM), hbm, hbm, *[vmem] * len(pieces)]
    aliases = {}
    if not first:
        if not last:
            aliases = {len(operands): 0}
        operands += state
        specs += [vmem, vmem]
    scratch = [pltpu.VMEM((blocks, columns, width), pieces[0].dtype)]
    if last:
        operands.append(own)
        specs.append(vmem)
        out_shape = jax.ShapeDtypeStruct((2 * half // own.shape[1], columns // 2), F32)
        out_specs = vmem
        scratch.append(pltpu.VMEM((2 * half, columns), F32))
    else:
        out_shape = (
            jax.ShapeDtypeStruct((2 * half, columns), F32),
            jax.ShapeDtypeStruct((2 * len(after), half, width), w_own.dtype),
        )
        out_specs = (vmem, vmem)
        scratch.append(pltpu.SemaphoreType.DMA((2 * len(after),)))
        if first:
            scratch.append(pltpu.VMEM((2 * blocks, half, width), w_own.dtype))
            scratch.append(pltpu.SemaphoreType.DMA((2 * blocks,)))
    return pl.pallas_call(
        functools.partial(
            block_products, numbers=numbers, after=after, first=first, last=last
        ),
        out_shape=out_shape,
        in_specs=specs,
        out_specs=out_specs,
        scratch_shapes=scratch,
        input_output_aliases=aliases,
        compiler_params=pltpu.CompilerParams(vmem_limit_bytes=VMEM_LIMIT),
        cost_estimate=pl.CostEstimate(
            flops=4 * blocks * half * columns * width,
            bytes_accessed=4 * blocks * half * width,
            transcendentals=0,
        ),
        name="block_products",
    )(*operands)


def node_factor(node_freq, node_weight, band_energy, energy_grid, pair_band):
    band_onehot = (
        pair_band[:, None] == jnp.arange(band_energy.shape[0], dtype=jnp.int32)[None, :]
    ).astype(F32)
    pair_eps = jnp.dot(band_onehot, band_energy, precision=lax.Precision.HIGHEST)
    delta = energy_grid[:, None] - pair_eps[None, :]
    return (
        node_weight[:, None, None]
        * delta[None]
        / (delta[None] ** 2 + node_freq[:, None, None] ** 2)
    )


def states_kernel(forms, factor, onehot, out):
    nodes, pairs = factor.shape[0], forms.shape[2]
    halves = factor.shape[2] // pairs
    form = jnp.sum(forms[...], axis=0)
    for part in range(2):
        total = None
        for h in range(halves):
            spot = pl.ds(h * pairs, pairs)
            row = 2 * nodes * h + part
            terms = form[row : row + 1, :] * factor[0, :, spot]
            for node in range(1, nodes):
                row = 2 * (nodes * h + node) + part
                terms += form[row : row + 1, :] * factor[node, :, spot]
            term = lax.dot_general(
                onehot[:, spot],
                terms,
                (((1,), (1,)), ((), ())),
                precision=lax.Precision.HIGHEST,
                preferred_element_type=F32,
            )
            total = term if total is None else total + term
        out[part] = total


def per_state(forms, factor, onehot):
    vmem = pl.BlockSpec(memory_space=pltpu.VMEM)
    return pl.pallas_call(
        states_kernel,
        out_shape=jax.ShapeDtypeStruct((2, onehot.shape[0], factor.shape[1]), F32),
        in_specs=[vmem] * 3,
        out_specs=vmem,
        compiler_params=pltpu.CompilerParams(vmem_limit_bytes=VMEM_LIMIT),
        name="per_state",
    )(forms, factor, onehot)


def per_device(
    screened, elements, node_freq, node_weight, band_energy, energy_grid, pair_state, pair_band
):
    nodes, _, depth, waves = screened.shape
    npair = elements.shape[1]
    half = npair // lax.axis_size("freq")
    core = lax.axis_index("freq")
    z, x = lax.axis_index("row_0"), lax.axis_index("row_1")
    nz, nx = lax.axis_size("row_0"), lax.axis_size("row_1")

    w_own = screened.reshape(nodes * 2 * depth, waves)
    w_other = shift(w_own, "freq", 1)
    w_own = pltpu.with_memory_space_constraint(w_own, pltpu.HBM)
    w_other = pltpu.with_memory_space_constraint(w_other, pltpu.HBM)

    mine = lax.dynamic_slice_in_dim(elements, core * half, half, 1)
    piece = mine.reshape(2 * half, depth)
    before = shift(piece, "row_1", 1)
    after = shift(piece, "row_1", -1)
    across = shift(piece, "row_1", 2)
    steps = jnp.arange(nz + 5, dtype=jnp.int32)
    offset = steps - nz
    offset = jnp.where(offset == 1, nx // 2, jnp.where(offset == 2, nx - 1, offset // 3))
    place = jnp.where(steps < nz, (z + steps) % nz, (x + offset) % nx)
    place = jnp.where(steps == nz + 4, core, place)

    factor = node_factor(node_freq, node_weight, band_energy, energy_grid, pair_band)
    state_onehot = (
        jnp.arange(NSTATE, dtype=jnp.int32)[:, None] == pair_state[None, :]
    ).astype(F32)

    far = nz // 2
    up = [jnp.concatenate([piece, across]), jnp.concatenate([before, after])]
    down = list(up)
    numbers, pieces, state = (0,), list(up), None
    for r in range(1, far):
        up = [shift(v, "row_0", 1) for v in up]
        down = [shift(v, "row_0", -1) for v in down]
        state = add_blocks(state, place, numbers, (nz - r, r), w_own, w_other, pieces)
        if r < far - 1:
            up[0], down[0], state = lax.optimization_barrier((up[0], down[0], state))
        numbers, pieces = (), []
        if r == 3:
            up[1], down[1], factor, state_onehot = lax.optimization_barrier(
                (up[1], down[1], factor, state_onehot)
            )
        numbers += (nz - r, r)
        pieces += [*up, *down]
    opposite = [shift(up[0], "row_0", 1), shift(down[1], "row_0", -1)]
    state = add_blocks(state, place, numbers, (far,), w_own, w_other, pieces)
    form = add_blocks(state, place, (far,), (), w_own, w_other, opposite, piece)

    sent = jnp.broadcast_to(form, (nx, *form.shape)).reshape(-1, 2 * nodes, half)
    form = lax.all_to_all(sent, ("row_1", "freq"), split_axis=0, concat_axis=0, tiled=True)
    form = form.reshape(nx, -1, half).sum(axis=0)
    forms = lax.all_to_all(
        jnp.broadcast_to(form, (nz, *form.shape)), "row_0", split_axis=0, concat_axis=0, tiled=True
    )
    sigma = per_state(forms, factor, state_onehot)
    return sigma + shift(sigma, "freq", 1)


def solution(mesh):
    split = Mesh(
        mesh.devices.reshape(mesh.shape["kpt"], 16, 4, mesh.shape["freq"]),
        ("kpt", "row_0", "row_1", "freq"),
    )
    return jax.shard_map(
        per_device,
        mesh=split,
        in_specs=(
            P(("kpt", "freq"), None, ROW, None),
            P(None, "kpt", ROW),
            P("freq"),
            P("freq"),
            P("kpt"),
            P(),
            P("kpt"),
            P("kpt"),
        ),
        out_specs=P(None, "kpt", None),
        check_vma=False,
    )
```

```python
import functools

import jax
import jax.numpy as jnp
from jax import lax
from jax.experimental import pallas as pl
from jax.experimental.pallas import tpu as pltpu
from jax.sharding import Mesh
from jax.sharding import PartitionSpec as P

NSTATE = 32
ROW = ("row_0", "row_1")
F32 = jnp.float32
VMEM_LIMIT = 20 * 2**20
CHUNK = 256
STEPS = 4


def shift(value, axis, step):
    size = lax.axis_size(axis)
    return lax.ppermute(value, axis, [(i, (i + step) % size) for i in range(size)])


def block_products(place, w_own, w_other, *refs, numbers, after, first, last):
    blocks = len(numbers)
    pieces = refs[: 2 * blocks]
    refs = refs[2 * blocks :]
    if not first:
        y_in, w_now, refs = refs[0], refs[1], refs[2:]
    if last:
        own, out, m_buf, y = refs
    elif first:
        y, w_next, m_buf, sems, w_now, first_sems = refs
    else:
        y, w_next, m_buf, sems = refs
    rows, width = w_own.shape[0], m_buf.shape[2]
    columns, lanes = m_buf.shape[1], pieces[0].shape[1]

    def reads(target, wanted, semaphores):
        return [
            pltpu.make_async_copy(
                w.at[:, pl.ds(pl.multiple_of(place[number] * width, width), width)],
                target.at[2 * b + half],
                semaphores.at[2 * b + half],
            )
            for b, number in enumerate(wanted)
            for half, w in enumerate((w_own, w_other))
        ]

    now = reads(w_now, numbers, first_sems) if first else []
    ahead = [] if last else reads(w_next, after, sems)
    for copy in now + ahead:
        copy.start()
    @pl.loop(0, STEPS)
    def _(i):
        count = columns // STEPS
        row = pl.multiple_of(i * count, count)
        for b in range(blocks):
            for k in range(4):
                lane = pl.multiple_of(place[place.shape[0] - 5 + k] * lanes, lanes)
                piece = pieces[2 * b + k // 2]
                m_buf[b, pl.ds(row, count), pl.ds(lane, lanes)] = piece[
                    pl.ds(k % 2 * columns + row, count), :
                ]

    if last:
        flat = own[...].astype(F32).T
        pairs, depth = columns // 2, own.shape[1]
        own_re, own_im = flat[:, :pairs], flat[:, pairs:]
    for copy in now:
        copy.wait()

    @pl.loop(0, 2 * rows // CHUNK)
    def _(i):
        half = i // (rows // CHUNK)
        row = pl.multiple_of(i % (rows // CHUNK) * CHUNK, CHUNK)
        spot = pl.ds(pl.multiple_of(i * CHUNK, CHUNK), CHUNK)
        total = None if first else y_in[spot, :]
        for b in range(blocks):
            term = lax.dot_general(
                w_now[2 * b + half, pl.ds(row, CHUNK), :],
                m_buf[b],
                (((1,), (1,)), ((), ())),
                preferred_element_type=F32,
            )
            total = term if total is None else total + term
        y[spot, :] = total

    if last:
        per_core = out.shape[0] // 4

        @pl.loop(0, out.shape[0] // 2)
        def _(node):
            base = pl.multiple_of(node * 2 * depth, 2 * depth)
            w_re = y[pl.ds(base, depth), :]
            w_im = y[pl.ds(base + depth, depth), :]
            y_re = w_re[:, :pairs] - w_im[:, pairs:]
            y_im = w_re[:, pairs:] + w_im[:, :pairs]
            form_re = jnp.sum(own_re * y_re + own_im * y_im, axis=0, keepdims=True)
            form_im = jnp.sum(own_re * y_im - own_im * y_re, axis=0, keepdims=True)
            half = (node // per_core + place[place.shape[0] - 1]) % 2
            spot = 2 * (half * per_core + node % per_core)
            out[pl.ds(spot, 1), :] = form_re
            out[pl.ds(spot + 1, 1), :] = form_im

    for copy in ahead:
        copy.wait()


def add_blocks(state, place, numbers, after, w_own, w_other, pieces, own=None):
    blocks = len(numbers)
    first, last = state is None, own is not None
    half, columns, width = w_own.shape[0], pieces[0].shape[0] // 2, 4 * pieces[0].shape[1]
    vmem = pl.BlockSpec(memory_space=pltpu.VMEM)
    hbm = pl.BlockSpec(memory_space=pltpu.HBM)
    operands = [place, w_own, w_other, *pieces]
    specs = [pl.BlockSpec(memory_space=pltpu.SMEM), hbm, hbm, *[vmem] * len(pieces)]
    aliases = {}
    if not first:
        if not last:
            aliases = {len(operands): 0}
        operands += state
        specs += [vmem, vmem]
    scratch = [pltpu.VMEM((blocks, columns, width), pieces[0].dtype)]
    if last:
        operands.append(own)
        specs.append(vmem)
        out_shape = jax.ShapeDtypeStruct((2 * half // own.shape[1], columns // 2), F32)
        out_specs = vmem
        scratch.append(pltpu.VMEM((2 * half, columns), F32))
    else:
        out_shape = (
            jax.ShapeDtypeStruct((2 * half, columns), F32),
            jax.ShapeDtypeStruct((2 * len(after), half, width), w_own.dtype),
        )
        out_specs = (vmem, vmem)
        scratch.append(pltpu.SemaphoreType.DMA((2 * len(after),)))
        if first:
            scratch.append(pltpu.VMEM((2 * blocks, half, width), w_own.dtype))
            scratch.append(pltpu.SemaphoreType.DMA((2 * blocks,)))
    return pl.pallas_call(
        functools.partial(
            block_products, numbers=numbers, after=after, first=first, last=last
        ),
        out_shape=out_shape,
        in_specs=specs,
        out_specs=out_specs,
        scratch_shapes=scratch,
        input_output_aliases=aliases,
        compiler_params=pltpu.CompilerParams(vmem_limit_bytes=VMEM_LIMIT),
        cost_estimate=pl.CostEstimate(
            flops=4 * blocks * half * columns * width,
            bytes_accessed=4 * blocks * half * width,
            transcendentals=0,
        ),
        name="block_products",
    )(*operands)


def node_factor(node_freq, node_weight, band_energy, energy_grid, pair_band):
    band_onehot = (
        pair_band[:, None] == jnp.arange(band_energy.shape[0], dtype=jnp.int32)[None, :]
    ).astype(F32)
    pair_eps = jnp.dot(band_onehot, band_energy, precision=lax.Precision.HIGHEST)
    delta = energy_grid[:, None] - pair_eps[None, :]
    return (
        node_weight[:, None, None]
        * delta[None]
        / (delta[None] ** 2 + node_freq[:, None, None] ** 2)
    )


def states_kernel(forms, factor, onehot, out):
    nodes, pairs = factor.shape[0], forms.shape[2]
    halves = factor.shape[2] // pairs
    form = jnp.sum(forms[...], axis=0)
    for part in range(2):
        total = None
        for h in range(halves):
            spot = pl.ds(h * pairs, pairs)
            row = 2 * nodes * h + part
            terms = form[row : row + 1, :] * factor[0, :, spot]
            for node in range(1, nodes):
                row = 2 * (nodes * h + node) + part
                terms += form[row : row + 1, :] * factor[node, :, spot]
            term = lax.dot_general(
                onehot[:, spot],
                terms,
                (((1,), (1,)), ((), ())),
                precision=lax.Precision.HIGHEST,
                preferred_element_type=F32,
            )
            total = term if total is None else total + term
        out[part] = total


def per_state(forms, factor, onehot):
    vmem = pl.BlockSpec(memory_space=pltpu.VMEM)
    return pl.pallas_call(
        states_kernel,
        out_shape=jax.ShapeDtypeStruct((2, onehot.shape[0], factor.shape[1]), F32),
        in_specs=[vmem] * 3,
        out_specs=vmem,
        compiler_params=pltpu.CompilerParams(vmem_limit_bytes=VMEM_LIMIT),
        name="per_state",
    )(forms, factor, onehot)


def per_device(
    screened, elements, node_freq, node_weight, band_energy, energy_grid, pair_state, pair_band
):
    nodes, _, depth, waves = screened.shape
    npair = elements.shape[1]
    half = npair // lax.axis_size("freq")
    core = lax.axis_index("freq")
    z, x = lax.axis_index("row_0"), lax.axis_index("row_1")
    nz, nx = lax.axis_size("row_0"), lax.axis_size("row_1")

    w_own = screened.reshape(nodes * 2 * depth, waves)
    w_other = shift(w_own, "freq", 1)
    w_own = pltpu.with_memory_space_constraint(w_own, pltpu.HBM)
    w_other = pltpu.with_memory_space_constraint(w_other, pltpu.HBM)

    mine = lax.dynamic_slice_in_dim(elements, core * half, half, 1)
    piece = mine.reshape(2 * half, depth)
    before = shift(piece, "row_1", 1)
    after = shift(piece, "row_1", -1)
    across = shift(piece, "row_1", 2)
    own_up, own_down = shift(piece, "row_0", 1), shift(piece, "row_0", -1)
    steps = jnp.arange(nz + 5, dtype=jnp.int32)
    offset = steps - nz
    offset = jnp.where(offset == 1, nx // 2, jnp.where(offset == 2, nx - 1, offset // 3))
    place = jnp.where(steps < nz, (z + steps) % nz, (x + offset) % nx)
    place = jnp.where(steps == nz + 4, core, place)

    factor = node_factor(node_freq, node_weight, band_energy, energy_grid, pair_band)
    state_onehot = (
        jnp.arange(NSTATE, dtype=jnp.int32)[:, None] == pair_state[None, :]
    ).astype(F32)

    far = nz // 2
    up = [jnp.concatenate([piece, across]), jnp.concatenate([before, after])]
    down = list(up)
    numbers, pieces, state = (0,), list(up), None
    for r in range(1, far):
        if r == 1:
            up = [jnp.concatenate([own_up, shift(across, "row_0", 1)]), shift(up[1], "row_0", 1)]
            down = [
                jnp.concatenate([own_down, shift(across, "row_0", -1)]),
                shift(down[1], "row_0", -1),
            ]
        else:
            up = [shift(v, "row_0", 1) for v in up]
            down = [shift(v, "row_0", -1) for v in down]
        state = add_blocks(state, place, numbers, (nz - r, r), w_own, w_other, pieces)
        if r < far - 1:
            up[0], down[0], state = lax.optimization_barrier((up[0], down[0], state))
        numbers, pieces = (), []
        if r == 3:
            up[1], down[1], factor, state_onehot = lax.optimization_barrier(
                (up[1], down[1], factor, state_onehot)
            )
        numbers += (nz - r, r)
        pieces += [*up, *down]
    opposite = [shift(up[0], "row_0", 1), shift(down[1], "row_0", -1)]
    state = add_blocks(state, place, numbers, (far,), w_own, w_other, pieces)
    form = add_blocks(state, place, (far,), (), w_own, w_other, opposite, piece)

    sent = jnp.broadcast_to(form, (nx, *form.shape)).reshape(-1, 2 * nodes, half)
    form = lax.all_to_all(sent, ("row_1", "freq"), split_axis=0, concat_axis=0, tiled=True)
    form = form.reshape(nx, -1, half).sum(axis=0)
    forms = lax.all_to_all(
        jnp.broadcast_to(form, (nz, *form.shape)), "row_0", split_axis=0, concat_axis=0, tiled=True
    )
    sigma = per_state(forms, factor, state_onehot)
    return sigma + shift(sigma, "freq", 1)


def solution(mesh):
    split = Mesh(
        mesh.devices.reshape(mesh.shape["kpt"], 16, 4, mesh.shape["freq"]),
        ("kpt", "row_0", "row_1", "freq"),
    )
    return jax.shard_map(
        per_device,
        mesh=split,
        in_specs=(
            P(("kpt", "freq"), None, ROW, None),
            P(None, "kpt", ROW),
            P("freq"),
            P("freq"),
            P("kpt"),
            P(),
            P("kpt"),
            P("kpt"),
        ),
        out_specs=P(None, "kpt", None),
        check_vma=False,
    )
```

```python
import functools

import jax
import jax.numpy as jnp
from jax import lax
from jax.experimental import pallas as pl
from jax.experimental.pallas import tpu as pltpu
from jax.sharding import Mesh
from jax.sharding import PartitionSpec as P

NSTATE = 32
ROW = ("row_0", "row_1")
F32 = jnp.float32
VMEM_LIMIT = 20 * 2**20


def shift(value, axis, step):
    size = lax.axis_size(axis)
    return lax.ppermute(value, axis, [(i, (i + step) % size) for i in range(size)])


def block_products(place, w_own, w_other, *refs, numbers, after, first, last):
    blocks = len(numbers)
    pieces = refs[: 2 * blocks]
    refs = refs[2 * blocks :]
    if not first:
        y_in, w_now, refs = refs[0], refs[1], refs[2:]
    if last:
        own, out, m_buf, y = refs
    elif first:
        y, w_next, m_buf, sems, w_now, first_sems = refs
    else:
        y, w_next, m_buf, sems = refs
    rows, width = w_own.shape[0], m_buf.shape[2]
    columns, lanes = m_buf.shape[1], pieces[0].shape[1]

    def reads(target, wanted, semaphores):
        return [
            pltpu.make_async_copy(
                w.at[:, pl.ds(pl.multiple_of(place[number] * width, width), width)],
                target.at[2 * b + half],
                semaphores.at[2 * b + half],
            )
            for b, number in enumerate(wanted)
            for half, w in enumerate((w_own, w_other))
        ]

    now = reads(w_now, numbers, first_sems) if first else []
    ahead = [] if last else reads(w_next, after, sems)
    for copy in now + ahead:
        copy.start()
    for b in range(blocks):
        for k in range(4):
            lane = pl.multiple_of(place[place.shape[0] - 5 + k] * lanes, lanes)
            piece = pieces[2 * b + k // 2]
            m_buf[b, :, pl.ds(lane, lanes)] = piece[pl.ds((k % 2) * columns, columns), :]
    if last:
        flat = own[...].astype(F32).T
        pairs, depth = columns // 2, own.shape[1]
        own_re, own_im = flat[:, :pairs], flat[:, pairs:]
    for copy in now:
        copy.wait()

    @pl.loop(0, 2)
    def _(half):
        spot = pl.ds(pl.multiple_of(half * rows, rows), rows)
        total = None if first else y_in[spot, :]
        for b in range(blocks):
            term = lax.dot_general(
                w_now[2 * b + half],
                m_buf[b],
                (((1,), (1,)), ((), ())),
                preferred_element_type=F32,
            )
            total = term if total is None else total + term
        y[spot, :] = total

    if last:
        per_core = out.shape[0] // 4

        @pl.loop(0, out.shape[0] // 2)
        def _(node):
            base = pl.multiple_of(node * 2 * depth, 2 * depth)
            w_re = y[pl.ds(base, depth), :]
            w_im = y[pl.ds(base + depth, depth), :]
            y_re = w_re[:, :pairs] - w_im[:, pairs:]
            y_im = w_re[:, pairs:] + w_im[:, :pairs]
            form_re = jnp.sum(own_re * y_re + own_im * y_im, axis=0, keepdims=True)
            form_im = jnp.sum(own_re * y_im - own_im * y_re, axis=0, keepdims=True)
            half = (node // per_core + place[place.shape[0] - 1]) % 2
            spot = 2 * (half * per_core + node % per_core)
            out[pl.ds(spot, 1), :] = form_re
            out[pl.ds(spot + 1, 1), :] = form_im

    for copy in ahead:
        copy.wait()


def add_blocks(state, place, numbers, after, w_own, w_other, pieces, own=None):
    blocks = len(numbers)
    first, last = state is None, own is not None
    half, columns, width = w_own.shape[0], pieces[0].shape[0] // 2, 4 * pieces[0].shape[1]
    vmem = pl.BlockSpec(memory_space=pltpu.VMEM)
    hbm = pl.BlockSpec(memory_space=pltpu.HBM)
    operands = [place, w_own, w_other, *pieces]
    specs = [pl.BlockSpec(memory_space=pltpu.SMEM), hbm, hbm, *[vmem] * len(pieces)]
    aliases = {}
    if not first:
        if not last:
            aliases = {len(operands): 0}
        operands += state
        specs += [vmem, vmem]
    scratch = [pltpu.VMEM((blocks, columns, width), pieces[0].dtype)]
    if last:
        operands.append(own)
        specs.append(vmem)
        out_shape = jax.ShapeDtypeStruct((2 * half // own.shape[1], columns // 2), F32)
        out_specs = vmem
        scratch.append(pltpu.VMEM((2 * half, columns), F32))
    else:
        out_shape = (
            jax.ShapeDtypeStruct((2 * half, columns), F32),
            jax.ShapeDtypeStruct((2 * len(after), half, width), w_own.dtype),
        )
        out_specs = (vmem, vmem)
        scratch.append(pltpu.SemaphoreType.DMA((2 * len(after),)))
        if first:
            scratch.append(pltpu.VMEM((2 * blocks, half, width), w_own.dtype))
            scratch.append(pltpu.SemaphoreType.DMA((2 * blocks,)))
    return pl.pallas_call(
        functools.partial(
            block_products, numbers=numbers, after=after, first=first, last=last
        ),
        out_shape=out_shape,
        in_specs=specs,
        out_specs=out_specs,
        scratch_shapes=scratch,
        input_output_aliases=aliases,
        compiler_params=pltpu.CompilerParams(vmem_limit_bytes=VMEM_LIMIT),
        cost_estimate=pl.CostEstimate(
            flops=4 * blocks * half * columns * width,
            bytes_accessed=4 * blocks * half * width,
            transcendentals=0,
        ),
        name="block_products",
    )(*operands)


def node_factor(node_freq, node_weight, band_energy, energy_grid, pair_band):
    band_onehot = (
        pair_band[:, None] == jnp.arange(band_energy.shape[0], dtype=jnp.int32)[None, :]
    ).astype(F32)
    pair_eps = jnp.dot(band_onehot, band_energy, precision=lax.Precision.HIGHEST)
    delta = energy_grid[:, None] - pair_eps[None, :]
    return (
        node_weight[:, None, None]
        * delta[None]
        / (delta[None] ** 2 + node_freq[:, None, None] ** 2)
    )


def states_kernel(forms, factor, onehot, out):
    nodes, pairs = factor.shape[0], forms.shape[2]
    halves = factor.shape[2] // pairs
    form = jnp.sum(forms[...], axis=0)
    for part in range(2):
        total = None
        for h in range(halves):
            spot = pl.ds(h * pairs, pairs)
            row = 2 * nodes * h + part
            terms = form[row : row + 1, :] * factor[0, :, spot]
            for node in range(1, nodes):
                row = 2 * (nodes * h + node) + part
                terms += form[row : row + 1, :] * factor[node, :, spot]
            term = lax.dot_general(
                onehot[:, spot],
                terms,
                (((1,), (1,)), ((), ())),
                precision=lax.Precision.HIGHEST,
                preferred_element_type=F32,
            )
            total = term if total is None else total + term
        out[part] = total


def per_state(forms, factor, onehot):
    vmem = pl.BlockSpec(memory_space=pltpu.VMEM)
    return pl.pallas_call(
        states_kernel,
        out_shape=jax.ShapeDtypeStruct((2, onehot.shape[0], factor.shape[1]), F32),
        in_specs=[vmem] * 3,
        out_specs=vmem,
        compiler_params=pltpu.CompilerParams(vmem_limit_bytes=VMEM_LIMIT),
        name="per_state",
    )(forms, factor, onehot)


def per_device(
    screened, elements, node_freq, node_weight, band_energy, energy_grid, pair_state, pair_band
):
    nodes, _, depth, waves = screened.shape
    npair = elements.shape[1]
    half = npair // lax.axis_size("freq")
    core = lax.axis_index("freq")
    z, x = lax.axis_index("row_0"), lax.axis_index("row_1")
    nz, nx = lax.axis_size("row_0"), lax.axis_size("row_1")

    w_own = screened.reshape(nodes * 2 * depth, waves)
    w_other = shift(w_own, "freq", 1)
    w_own = pltpu.with_memory_space_constraint(w_own, pltpu.HBM)
    w_other = pltpu.with_memory_space_constraint(w_other, pltpu.HBM)

    mine = lax.dynamic_slice_in_dim(elements, core * half, half, 1)
    piece = mine.reshape(2 * half, depth)
    before = shift(piece, "row_1", 1)
    after = shift(piece, "row_1", -1)
    onward, before, after = lax.optimization_barrier((piece, before, after))
    across = shift(onward, "row_1", 2)
    steps = jnp.arange(nz + 5, dtype=jnp.int32)
    offset = steps - nz
    offset = jnp.where(offset == 1, nx // 2, jnp.where(offset == 2, nx - 1, offset // 3))
    place = jnp.where(steps < nz, (z + steps) % nz, (x + offset) % nx)
    place = jnp.where(steps == nz + 4, core, place)

    factor = node_factor(node_freq, node_weight, band_energy, energy_grid, pair_band)
    state_onehot = (
        jnp.arange(NSTATE, dtype=jnp.int32)[:, None] == pair_state[None, :]
    ).astype(F32)

    far = nz // 2
    up = [jnp.concatenate([piece, across]), jnp.concatenate([before, after])]
    down = list(up)
    numbers, pieces, state = (0,), list(up), None
    for r in range(1, far):
        up = [shift(v, "row_0", 1) for v in up]
        down = [shift(v, "row_0", -1) for v in down]
        state = add_blocks(state, place, numbers, (nz - r, r), w_own, w_other, pieces)
        if r < far - 1:
            up[0], down[0], state = lax.optimization_barrier((up[0], down[0], state))
        numbers, pieces = (), []
        if r == 3:
            up[1], down[1], factor, state_onehot = lax.optimization_barrier(
                (up[1], down[1], factor, state_onehot)
            )
        numbers += (nz - r, r)
        pieces += [*up, *down]
    opposite = [shift(up[0], "row_0", 1), shift(down[1], "row_0", -1)]
    state = add_blocks(state, place, numbers, (far,), w_own, w_other, pieces)
    form = add_blocks(state, place, (far,), (), w_own, w_other, opposite, piece)

    sent = jnp.broadcast_to(form, (nx, *form.shape)).reshape(-1, 2 * nodes, half)
    form = lax.all_to_all(sent, ("row_1", "freq"), split_axis=0, concat_axis=0, tiled=True)
    form = form.reshape(nx, -1, half).sum(axis=0)
    forms = lax.all_to_all(
        jnp.broadcast_to(form, (nz, *form.shape)), "row_0", split_axis=0, concat_axis=0, tiled=True
    )
    sigma = per_state(forms, factor, state_onehot)
    return sigma + shift(sigma, "freq", 1)


def solution(mesh):
    split = Mesh(
        mesh.devices.reshape(mesh.shape["kpt"], 16, 4, mesh.shape["freq"]),
        ("kpt", "row_0", "row_1", "freq"),
    )
    return jax.shard_map(
        per_device,
        mesh=split,
        in_specs=(
            P(("kpt", "freq"), None, ROW, None),
            P(None, "kpt", ROW),
            P("freq"),
            P("freq"),
            P("kpt"),
            P(),
            P("kpt"),
            P("kpt"),
        ),
        out_specs=P(None, "kpt", None),
        check_vma=False,
    )
```
